256 devices in a mesh: cfg: 2 (over y_hi), seq: 16 (over z, core), tp: 8 (over y_lo, x).
Axes of the slice: x: 4, y: 4 (y_hi: 2, y_lo: 2; y = y_hi * 2 + y_lo), z: 8, core: 2. Of those that a mesh axis runs over, the one named last changes fastest.
Arguments:
- queries: bfloat16 [2, 7680, 5120], P('cfg', 'seq', 'tp'), may hold values from -5 to 5
- keys: bfloat16 [2, 7680, 5120], P('cfg', 'seq', 'tp'), may hold values from -5 to 5
- values: bfloat16 [2, 7680, 5120], P('cfg', 'seq', 'tp'), may hold values from -5 to 5
- text_keys: bfloat16 [2, 512, 5120], P('cfg', None, 'tp'), may hold values from -7.5 to 7.5
- text_values: bfloat16 [2, 512, 5120], P('cfg', None, 'tp'), may hold values from -5 to 5
- prompt_lengths: int32 [2], P('cfg'), may hold values from 64 to 512
- frame_counts: int32 [16], P('seq'), may hold values from 240 to 480
- out_weight: bfloat16 [5120, 5120], P('tp'), may hold values from -0.5 to 0.5
Outputs:
- velocity: bfloat16 [7680, 5120], P('seq', ('tp', 'cfg'))
The draws below stay inside these ranges and needn't reach their ends.
All inputs are finite; a program needn't handle non-finite values.
Results may differ from the reference program's by a relative error of at most 0.015.
Values may be sent and summed in bfloat16 or wider, within the bound.
No kernel may reach another device: no remote copies, remote signals or barrier semaphores. Data moves between devices by JAX's collectives and lax.ppermute only.
A program may use at most 256 MiB of HBM per device.

```python
import jax
import jax.numpy as jnp
from jax import lax

HEADS = 40
HEAD_DIM = 128
D = 5120
TEXT = 512
FRAME_SLOTS = 480
FRAMES = 16
TOKENS = 7680


def query_key_pair(key):
    base = jax.random.fold_in(key, 7)
    shape = (2, TOKENS, D)
    query_draw = jnp.clip(1.5 * jax.random.normal(jax.random.fold_in(base, 1), shape, jnp.float32), -5.0, 5.0)
    key_draw = jnp.clip(jax.random.normal(jax.random.fold_in(base, 2), shape, jnp.float32), -5.0, 5.0)
    return (query_draw, key_draw)


def draw_queries(key, part):
    return query_key_pair(key)[0].astype(jnp.bfloat16)


def draw_keys(key, part):
    return query_key_pair(key)[1].astype(jnp.bfloat16)


def touch_ends(entries, key, least, top_value):
    longest = entries.shape.index(max(entries.shape))
    spots = []
    for shift in (0, 1):
        where = [jax.random.randint(jax.random.fold_in(key, axis), (), 0, length) for axis, length in enumerate(entries.shape)]
        where[longest] = (where[longest] + shift) % entries.shape[longest]
        spots.append(tuple(where))
    return entries.at[spots[0]].set(least).at[spots[1]].set(top_value)


def levels(rng, shape, shards, smallest, high):
    def one(position, blocks):
        draws = jax.random.uniform(jax.random.fold_in(jax.random.fold_in(rng, 6), position), (blocks,), jnp.float32, smallest / len(shards), high / len(shards))
        return jnp.repeat(jnp.exp(draws), shape[position] // blocks).reshape((-1,) + (1,) * (len(shape) - position - 1))

    gain = one(*shards[0])
    for cut in shards[1:]:
        gain = gain * one(*cut)
    return gain


def normal_values(stream_key, extent, scale, limit, shards=(), kind=jnp.bfloat16):
    level = levels(stream_key, extent, shards, -0.22, 0.18) if shards else 1.0
    array = jax.random.normal(stream_key, extent, jnp.float32) * scale * level
    return jnp.minimum(jnp.maximum(array, -limit), limit).astype(kind)


def setup_inputs(seed: int = 0) -> dict:
    seeds = jax.random.split(jax.random.key(seed), 9)
    return {
        "queries": draw_queries(jax.random.fold_in(seeds[8], 71), 0),
        "keys": draw_keys(jax.random.fold_in(seeds[8], 71), 0),
        "values": normal_values(seeds[2], (2, TOKENS, D), 1.0, 5.0, ((0, 2), (1, 16), (2, 8))),
        "text_keys": normal_values(seeds[3], (2, TEXT, D), 1.5, 7.5, ((0, 2), (2, 8))),
        "text_values": normal_values(seeds[4], (2, TEXT, D), 1.0, 5.0, ((0, 2), (2, 8))),
        "prompt_lengths": jax.random.randint(seeds[5], (2,), TEXT // 8, TEXT + 1).astype(jnp.int32),
        "frame_counts": touch_ends(jax.random.randint(seeds[6], (FRAMES,), FRAME_SLOTS // 2, FRAME_SLOTS + 1), jax.random.fold_in(seeds[6], 1), FRAME_SLOTS // 2, FRAME_SLOTS).astype(jnp.int32),
        "out_weight": normal_values(seeds[7], (D, D), (D // 32) ** -0.5, 0.5, ((0, 8),)),
    }


GUIDANCE = 5.0
RESCALE = 0.7
NEGATIVE = -1e+30

def video_valid(frame_counts):
    positions = jnp.arange(TOKENS, dtype=jnp.int32)
    return positions % FRAME_SLOTS < frame_counts[positions // FRAME_SLOTS]

def branch_output(query_rows, key_rows, value_rows, text_key_rows, text_value_rows, length, video_mask, out_weight):
    text_mask = jnp.arange(TEXT, dtype=jnp.int32) < length
    full_mask = jnp.concatenate([text_mask, video_mask])
    all_keys = jnp.concatenate([text_key_rows, key_rows], axis=0)
    all_values = jnp.concatenate([text_value_rows, value_rows], axis=0)
    key_total = all_keys.shape[0]
    query_heads = jnp.transpose(query_rows.reshape(TOKENS, HEADS, HEAD_DIM), (1, 0, 2))
    key_heads = jnp.transpose(all_keys.reshape(key_total, HEADS, HEAD_DIM), (1, 0, 2))
    value_heads = jnp.transpose(all_values.reshape(key_total, HEADS, HEAD_DIM), (1, 0, 2))

    def one_head(operands):
        query_head, key_head, value_head = operands
        scores = jnp.dot(query_head, key_head.T, preferred_element_type=jnp.float32) * HEAD_DIM ** (-0.5)
        scores = jnp.where(full_mask[None, :], scores, NEGATIVE)
        row_max = lax.optimization_barrier(jnp.max(scores, axis=1, keepdims=True))
        weights = jnp.exp(scores - row_max)
        weight_sum = lax.optimization_barrier(jnp.sum(weights, axis=1, keepdims=True))
        mixed_rows = jnp.dot(weights.astype(jnp.bfloat16), value_head, preferred_element_type=jnp.float32)
        return (mixed_rows / weight_sum).astype(jnp.bfloat16)
    heads_out = lax.map(one_head, (query_heads, key_heads, value_heads))
    attended = jnp.transpose(heads_out, (1, 0, 2)).reshape(TOKENS, HEADS * HEAD_DIM)
    return jnp.dot(attended, out_weight, preferred_element_type=jnp.float32).astype(jnp.bfloat16)

def reference(queries, keys, values, text_keys, text_values, prompt_lengths, frame_counts, out_weight):
    video_mask = video_valid(frame_counts)
    conditional = branch_output(queries[0], keys[0], values[0], text_keys[0], text_values[0], prompt_lengths[0], video_mask, out_weight).astype(jnp.float32)
    unconditional = branch_output(queries[1], keys[1], values[1], text_keys[1], text_values[1], prompt_lengths[1], video_mask, out_weight).astype(jnp.float32)
    guided = unconditional + GUIDANCE * (conditional - unconditional)
    token_weights = video_mask.astype(jnp.float32)
    valid_total = jnp.sum(frame_counts).astype(jnp.float32)

    def moment(field_rows):
        return jnp.dot(token_weights, field_rows, precision=lax.Precision.HIGHEST) / valid_total
    guided_mean = moment(guided)
    guided_var = moment(guided * guided) - guided_mean * guided_mean
    cond_mean = moment(conditional)
    cond_var = moment(conditional * conditional) - cond_mean * cond_mean
    std_ratio = jnp.sqrt((cond_var + 1.0) / (guided_var + 1.0))
    factor = RESCALE * std_ratio + (1.0 - RESCALE)
    return (guided_mean + (guided - guided_mean) * factor).astype(jnp.bfloat16)
```

```python
import math

import jax
import jax.numpy as jnp
from jax import lax
from jax.experimental import pallas as pl
from jax.experimental.pallas import tpu as pltpu
from jax.sharding import PartitionSpec as P


HEAD_DIM = 128
FRAME_SLOTS = 480
LEAST_FRAME = 240
LEAST_PROMPT = 64

GUIDANCE = 5.0
RESCALE = 0.7
NEGATIVE = -1e30
LOG2_SCALE = math.log2(math.e) * HEAD_DIM ** (-0.5)

GROUPS = ((0, 3), (3, 2))

CALLS = (
    (("f1", "b1", "f2", "b2"), ("sn",), ("f3", "b3", "sf3", "sb3"), ("l4", "sl4")),
    (("f1", "b1"), ("sn", "f2", "b2"), ("sf2", "sb2", "b3", "sb3"), ("f3", "sf3", "l4", "sl4")),
)


CORE_SWAP = [(i, i ^ 1) for i in range(16)]


def z_shift(step):
    return [(z * 2 + c, ((z + step) % 8) * 2 + c) for z in range(8) for c in range(2)]


def tp_index(y, x):
    return (y % 2) * 4 + x % 4


def tp_shift(dy, dx):
    return [(tp_index(y, x), tp_index(y + dy, x + dx)) for y in range(2) for x in range(4)]


def weight_round(step):
    pairs = []
    for s in range(16):
        for y in range(2):
            for x in range(4):
                target = tp_index(y + 1, x) if step == 3 else tp_index(y + s % 2, x + step + 1)
                pairs.append((s * 8 + tp_index(y, x), s * 8 + target))
    return pairs


def with_count(pair, frame_count):
    high = jnp.full((2, 8, pair.shape[2]), frame_count // 16, jnp.int32).astype(pair.dtype)
    low = jnp.full((2, 8, pair.shape[2]), frame_count % 16, jnp.int32).astype(pair.dtype)
    return jnp.concatenate([pair, high, low], axis=1)


def count_of(rows):
    values = rows.astype(jnp.float32)
    return (values[0:1, 0:1] * 16.0 + values[8:9, 0:1]).astype(jnp.int32)


def frame_piece(ref):
    return (
        lambda: ref[0, :FRAME_SLOTS],
        lambda: ref[1, :FRAME_SLOTS],
        lambda: count_of(ref[0, FRAME_SLOTS:]),
        LEAST_FRAME,
    )


def scores_of(key_rows, query_rows):
    return lax.dot_general(
        key_rows, query_rows, (((1,), (1,)), ((), ())), preferred_element_type=jnp.float32
    )


def attend(query, limits, items, state, final, first, width, state_at=0, emit=False):
    rows = query.shape[0]
    heads = width
    has_state = state is not None
    kinds = []
    operands = []
    specs = []
    for kind, arrays in items:
        if kind == "text":
            kinds.append((kind, 1))
            for a in arrays:
                operands.append(a)
                specs.append(pl.BlockSpec((a.shape[0], HEAD_DIM), lambda h: (0, h + first)))
        elif kind == "stack":
            kinds.append((kind, arrays.shape[0]))
            operands.append(arrays)
            shape = (arrays.shape[0], 2, arrays.shape[2], HEAD_DIM)
            specs.append(pl.BlockSpec(shape, lambda h: (0, 0, 0, h)))
        else:
            kinds.append((kind, 1))
            operands.append(arrays)
            at = first if kind == "all" else 0
            specs.append(pl.BlockSpec((2, arrays.shape[1], HEAD_DIM), lambda h, at=at: (0, 0, h + at)))
    max_spec = pl.BlockSpec((None, 8, rows), lambda h: (h, 0, 0))
    mix_spec = pl.BlockSpec((None, HEAD_DIM, rows), lambda h: (h, 0, 0))
    state_specs = [max_spec, max_spec, mix_spec]
    at_state = state_at
    given_specs = [
        pl.BlockSpec((None, 8, rows), lambda h: (h + at_state, 0, 0)),
        pl.BlockSpec((None, 8, rows), lambda h: (h + at_state, 0, 0)),
        pl.BlockSpec((None, HEAD_DIM, rows), lambda h: (h + at_state, 0, 0)),
    ]
    state_shapes = [
        jax.ShapeDtypeStruct((heads, 8, rows), jnp.float32),
        jax.ShapeDtypeStruct((heads, 8, rows), jnp.float32),
        jax.ShapeDtypeStruct((heads, HEAD_DIM, rows), jnp.float32),
    ]
    if final:
        out_specs = pl.BlockSpec((rows, HEAD_DIM), lambda h: (0, h))
        out_shape = jax.ShapeDtypeStruct((rows, heads * HEAD_DIM), jnp.bfloat16)
    else:
        out_specs, out_shape = list(state_specs), list(state_shapes)
        if emit:
            slots = items[0][1].shape[1]
            out_specs.append(
                pl.BlockSpec((len(items), 2, slots, HEAD_DIM), lambda h: (0, 0, 0, h))
            )
            out_shape.append(
                jax.ShapeDtypeStruct((len(items), 2, slots, heads * HEAD_DIM), jnp.bfloat16)
            )

    def kernel(limit_ref, query_ref, *refs):
        given = list(refs)
        if has_state:
            max_ref, sum_ref, mix_ref = given[:3]
            given = given[3:]
        pieces, copied = [], []
        for kind, count in kinds:
            if kind == "text":
                k_ref, v_ref = given[:2]
                given = given[2:]
                pieces.append(
                    (lambda r=k_ref: r[...], lambda r=v_ref: r[...], None, LEAST_PROMPT)
                )
            else:
                r = given.pop(0)
                if kind == "block":
                    copied.append(r)
                if kind == "stack":
                    pieces += [frame_piece(r.at[i]) for i in range(count)]
                else:
                    pieces.append(frame_piece(r))
        outs = given
        q = query_ref[...]
        if has_state:
            carry = (max_ref[0:1], sum_ref[0:1], mix_ref[...])
        else:
            carry = (
                jnp.full((1, rows), NEGATIVE, jnp.float32),
                jnp.zeros((1, rows), jnp.float32),
                jnp.zeros((HEAD_DIM, rows), jnp.float32),
            )

        def run(pieces, carry):
            row_max, weight_sum, mixed = carry
            scores = scores_of(pieces[0][0](), q)
            for i, (_, value_of, limit_of, sure) in enumerate(pieces):
                ahead = scores_of(pieces[i + 1][0](), q) if i + 1 < len(pieces) else None
                count = scores.shape[0]
                slots = lax.broadcasted_iota(jnp.int32, (count - sure, rows), 0) + sure
                limit = limit_ref[0] if limit_of is None else limit_of()
                tail = jnp.where(slots < limit, scores[sure:], NEGATIVE)
                scores = jnp.concatenate([scores[:sure], tail], axis=0)
                new_max = jnp.maximum(row_max, jnp.max(scores, axis=0, keepdims=True))
                base = new_max * LOG2_SCALE
                weights = jnp.exp2(scores * LOG2_SCALE - base)
                shrink = jnp.exp2(row_max * LOG2_SCALE - base)
                columns = jnp.concatenate(
                    [value_of().T, jnp.ones((16, count), jnp.bfloat16)], axis=0
                )
                added = jnp.dot(
                    columns, weights.astype(jnp.bfloat16), preferred_element_type=jnp.float32
                )
                weight_sum = weight_sum * shrink + added[HEAD_DIM : HEAD_DIM + 1]
                mixed = mixed * shrink + added[:HEAD_DIM]
                row_max = new_max
                scores = ahead
            return row_max, weight_sum, mixed

        for i, r in enumerate(copied):
            outs[3][i] = r[...]
        carry = run(pieces, carry)
        row_max, weight_sum, mixed = carry
        if final:
            outs[0][...] = (mixed / weight_sum).T.astype(jnp.bfloat16)
        else:
            outs[0][...] = jnp.broadcast_to(row_max, (8, rows))
            outs[1][...] = jnp.broadcast_to(weight_sum, (8, rows))
            outs[2][...] = mixed

    keys_total = sum(512 if k == "text" else n * FRAME_SLOTS for k, n in kinds)
    flops = 4 * rows * keys_total * HEAD_DIM * heads
    return pl.pallas_call(
        kernel,
        grid=(heads,),
        in_specs=[
            pl.BlockSpec(memory_space=pltpu.SMEM),
            pl.BlockSpec((rows, HEAD_DIM), lambda h: (0, h + first)),
            *(given_specs if has_state else []),
            *specs,
        ],
        out_specs=out_specs,
        out_shape=out_shape,
        compiler_params=pltpu.CompilerParams(vmem_limit_bytes=24 << 20),
        cost_estimate=pl.CostEstimate(
            flops=flops * 2, transcendentals=rows * keys_total * heads, bytes_accessed=1 << 20
        ),
    )(limits, query, *(state if has_state else ()), *operands)


def project(place, total, entries, steps, weights, rows, features, final):
    has_total = total is not None

    def kernel(place_ref, *refs):
        given = list(refs)
        total_ref = given.pop(0) if has_total else None
        h = pl.program_id(0)
        north = place_ref[0] == 0
        result = None
        for _ in entries:
            a, w = given[:8], given[8:16]
            given = given[16:]
            blocks = [a[0][...], a[1][...]]
            for x, y in ((2, 3), (4, 5), (6, 7)):
                blocks.append(jnp.where(north, a[x][...], a[y][...]))
            for x, y in ((2, 3), (4, 5), (6, 7)):
                blocks.append(jnp.where(north, a[y][...], a[x][...]))
            part = jnp.dot(
                jnp.concatenate(blocks, axis=1),
                jnp.concatenate([r[...] for r in w], axis=0),
                preferred_element_type=jnp.float32,
            )
            result = part if result is None else result + part
        if final:
            result = (total_ref[...] + result).astype(jnp.bfloat16)
            lower, upper = result[:, : features // 2], result[:, features // 2 :]
            given[0][...] = jnp.where(place_ref[1] == 0, lower, upper)
            given[1][...] = jnp.where(place_ref[1] == 0, upper, lower)
            return
        out = given[0]

        @pl.when(h == 0)
        def _():
            out[...] = result

        if steps > 1:
            @pl.when(h > 0)
            def _():
                out[...] = out[...] + result

    operands, specs = [], []
    for attended, first, at in entries:
        operands += [*attended, *weights]
        specs += [pl.BlockSpec((rows, HEAD_DIM), lambda h, at=at: (0, h + at))] * len(attended)
        specs += [pl.BlockSpec((HEAD_DIM, features), lambda h, first=first: (h + first, 0))] * len(weights)
    whole = pl.BlockSpec((rows, features), lambda h: (0, 0))
    flops = 16 * rows * features * HEAD_DIM * steps * len(entries)
    return pl.pallas_call(
        kernel,
        grid=(steps,),
        in_specs=[
            pl.BlockSpec(memory_space=pltpu.SMEM),
            *([whole] if has_total else []),
            *specs,
        ],
        out_specs=[pl.BlockSpec((rows, features // 2), lambda h: (0, 0))] * 2 if final else whole,
        out_shape=[jax.ShapeDtypeStruct((rows, features // 2), jnp.bfloat16)] * 2
        if final
        else jax.ShapeDtypeStruct((rows, features), jnp.float32),
        compiler_params=pltpu.CompilerParams(vmem_limit_bytes=24 << 20),
        cost_estimate=pl.CostEstimate(flops=flops, transcendentals=0, bytes_accessed=1 << 20),
    )(place, *([total] if has_total else []), *operands)


def step(queries, keys, values, text_keys, text_values, prompt_lengths, frame_counts, out_weight):
    query, text_k, text_v = queries[0], text_keys[0], text_values[0]
    head_total = query.shape[1] // HEAD_DIM
    rows = query.shape[0]
    features = out_weight.shape[1] // lax.axis_size("tp")
    seq = lax.axis_index("seq")
    tp = lax.axis_index("tp")
    cfg = lax.axis_index("cfg")
    core = seq % 2

    def send(x, axis, pairs):
        return lax.ppermute(x, axis, pairs)

    limits = prompt_lengths

    def rows_of(first, heads):
        cols = slice(first * HEAD_DIM, (first + heads) * HEAD_DIM)
        return with_count(jnp.stack([keys[0][:, cols], values[0][:, cols]]), frame_counts[0])

    both_rows = rows_of(0, head_total)
    both_swapped = send(both_rows, "seq", CORE_SWAP)

    x_pos, y_pos = tp % 4, tp // 4

    def columns_for(target):
        return lax.dynamic_slice(out_weight, (0, target * features), (out_weight.shape[0], features))

    got, got_swapped = [], []
    for step in range(4):
        if step == 3:
            target = (1 - y_pos) * 4 + x_pos
        else:
            target = ((y_pos + core) % 2) * 4 + (x_pos + step + 1) % 4
        got.append(send(columns_for(target), ("seq", "tp"), weight_round(step)))
    for step in range(3):
        got_swapped.append(send(got[step], "seq", CORE_SWAP))
    weights = (columns_for(tp), got[3], *got[:3], *got_swapped)

    start_state = attend(
        query,
        limits,
        [("text", (text_k, text_v)), ("all", both_rows), ("all", both_swapped)],
        None,
        False,
        0,
        head_total,
    )

    rings = []
    for g, (first, heads) in enumerate(GROUPS):
        own = rows_of(first, heads)
        forward, backward = [own], [own]
        for _ in range(3):
            forward.append(send(forward[-1], "seq", z_shift(1)))
            backward.append(send(backward[-1], "seq", z_shift(-1)))
        last = send(backward[3], "seq", z_shift(-1)) if g == 1 else send(forward[3], "seq", z_shift(1))
        frames = {"l4": last}
        for i in (1, 2, 3):
            frames["f%d" % i] = forward[i]
            frames["b%d" % i] = backward[i]
        calls = CALLS[g]
        *state, stacked = attend(
            query,
            limits,
            [("block", frames[name]) for name in calls[0]],
            start_state,
            False,
            first,
            heads,
            first,
            True,
        )
        frames["sn"] = send(stacked, "seq", CORE_SWAP)
        for name in sum(calls[1:], ()):
            if name not in frames:
                frames[name] = send(frames[name[1:]], "seq", CORE_SWAP)
        rings.append((state, frames))

    gathered = []
    place = jnp.stack([core, cfg]).astype(jnp.int32)
    for g, ((first, heads), (state, frames)) in enumerate(zip(GROUPS, rings)):
        for i, names in enumerate(CALLS[g][1:]):
            items = [("stack" if name == "sn" else "last", frames[name]) for name in names]
            final = i + 2 == len(CALLS[g])
            state = attend(query, limits, items, state, final, first, heads)
        mine = state

        def near_tp(x, dy, dx):
            return send(x, "tp", tp_shift(dy, dx))

        across = near_tp(mine, 1, 0)
        left = near_tp(mine, 0, 1)
        right = near_tp(mine, 0, -1)
        left_a = near_tp(across, 0, 1)
        right_a = near_tp(across, 0, -1)
        far = near_tp(left, 0, 1)
        far_a = near_tp(right_a, 0, -1)
        attended = [mine, across, left, left_a, far, far_a, right, right_a]
        gathered.append(attended)
    total = project(place, None, [(gathered[0], 0, 0)], GROUPS[0][1], weights, rows, features, False)
    first, heads = GROUPS[1]
    entries = [(gathered[1], first + i, i) for i in range(heads)]
    total = project(place, total, entries, 1, weights, rows, features, True)

    half = features // 2
    kept, leaving = total
    given = send(leaving, "cfg", [(0, 1), (1, 0)])
    conditional = jnp.where(cfg == 0, kept, given).astype(jnp.float32)
    unconditional = jnp.where(cfg == 0, given, kept).astype(jnp.float32)
    guided = unconditional + GUIDANCE * (conditional - unconditional)
    token_weights = (jnp.arange(rows, dtype=jnp.int32) < frame_counts[0]).astype(jnp.float32)[:, None]

    def local_sum(field):
        return jnp.sum(field * token_weights, axis=0)

    sums = jnp.stack(
        [
            local_sum(guided),
            local_sum(guided * guided),
            local_sum(conditional),
            local_sum(conditional * conditional),
            jnp.broadcast_to(frame_counts.astype(jnp.float32), (half,)),
        ]
    )
    for bit in (1, 2, 4, 8):
        sums = sums + send(sums, "seq", [(i, i ^ bit) for i in range(16)])
    valid_total = sums[4]
    guided_mean = sums[0] / valid_total
    guided_var = sums[1] / valid_total - guided_mean * guided_mean
    cond_mean = sums[2] / valid_total
    cond_var = sums[3] / valid_total - cond_mean * cond_mean
    std_ratio = jnp.sqrt((cond_var + 1.0) / (guided_var + 1.0))
    factor = RESCALE * std_ratio + (1.0 - RESCALE)
    return (guided_mean + (guided - guided_mean) * factor).astype(jnp.bfloat16)


def solution(mesh):
    placed = (
        P("cfg", "seq", "tp"),
        P("cfg", "seq", "tp"),
        P("cfg", "seq", "tp"),
        P("cfg", None, "tp"),
        P("cfg", None, "tp"),
        P("cfg"),
        P("seq"),
        P("tp", None),
    )
    return jax.shard_map(step, mesh=mesh, in_specs=placed, out_specs=P("seq", ("tp", "cfg")), check_vma=False)
```

```python
import math

import jax
import jax.numpy as jnp
from jax import lax
from jax.experimental import pallas as pl
from jax.experimental.pallas import tpu as pltpu
from jax.sharding import PartitionSpec as P


HEAD_DIM = 128
FRAME_SLOTS = 480
LEAST_FRAME = 240
LEAST_PROMPT = 64

GUIDANCE = 5.0
RESCALE = 0.7
NEGATIVE = -1e30
LOG2_SCALE = math.log2(math.e) * HEAD_DIM ** (-0.5)

GROUPS = ((0, 3), (3, 2))

CALLS = (
    (("f1", "b1", "f2", "b2"), ("sn",), ("f3", "b3", "sf3", "sb3"), ("l4", "sl4")),
    (("f1", "b1"), ("sn", "f2", "b2"), ("sf2", "sb2", "b3", "sb3"), ("f3", "sf3", "l4", "sl4")),
)


CORE_SWAP = [(i, i ^ 1) for i in range(16)]


def z_shift(step):
    return [(z * 2 + c, ((z + step) % 8) * 2 + c) for z in range(8) for c in range(2)]


def tp_index(y, x):
    return (y % 2) * 4 + x % 4


def tp_shift(dy, dx):
    return [(tp_index(y, x), tp_index(y + dy, x + dx)) for y in range(2) for x in range(4)]


def weight_round(step):
    pairs = []
    for s in range(16):
        for y in range(2):
            for x in range(4):
                target = tp_index(y + 1, x) if step == 3 else tp_index(y + s % 2, x + step + 1)
                pairs.append((s * 8 + tp_index(y, x), s * 8 + target))
    return pairs


def with_count(pair, frame_count):
    high = jnp.full((2, 8, pair.shape[2]), frame_count // 16, jnp.int32).astype(pair.dtype)
    low = jnp.full((2, 8, pair.shape[2]), frame_count % 16, jnp.int32).astype(pair.dtype)
    return jnp.concatenate([pair, high, low], axis=1)


def count_of(rows):
    values = rows.astype(jnp.float32)
    return (values[0:1, 0:1] * 16.0 + values[8:9, 0:1]).astype(jnp.int32)


def frame_piece(ref):
    return (
        lambda: ref[0, :FRAME_SLOTS],
        lambda: ref[1, :FRAME_SLOTS],
        lambda: count_of(ref[0, FRAME_SLOTS:]),
        LEAST_FRAME,
    )


def scores_of(key_rows, query_rows):
    return lax.dot_general(
        key_rows, query_rows, (((1,), (1,)), ((), ())), preferred_element_type=jnp.float32
    )


def attend(query, limits, items, state, final, first, width, state_at=0, emit=False):
    rows = query.shape[0]
    heads = width
    has_state = state is not None
    kinds = []
    operands = []
    specs = []
    for kind, arrays in items:
        if kind == "text":
            kinds.append((kind, 1))
            for a in arrays:
                operands.append(a)
                specs.append(pl.BlockSpec((a.shape[0], HEAD_DIM), lambda h: (0, h + first)))
        elif kind == "stack":
            kinds.append((kind, arrays.shape[0]))
            operands.append(arrays)
            shape = (arrays.shape[0], 2, arrays.shape[2], HEAD_DIM)
            specs.append(pl.BlockSpec(shape, lambda h: (0, 0, 0, h)))
        else:
            kinds.append((kind, 1))
            operands.append(arrays)
            at = first if kind == "all" else 0
            specs.append(pl.BlockSpec((2, arrays.shape[1], HEAD_DIM), lambda h, at=at: (0, 0, h + at)))
    max_spec = pl.BlockSpec((None, 8, rows), lambda h: (h, 0, 0))
    mix_spec = pl.BlockSpec((None, HEAD_DIM, rows), lambda h: (h, 0, 0))
    state_specs = [max_spec, max_spec, mix_spec]
    at_state = state_at
    given_specs = [
        pl.BlockSpec((None, 8, rows), lambda h: (h + at_state, 0, 0)),
        pl.BlockSpec((None, 8, rows), lambda h: (h + at_state, 0, 0)),
        pl.BlockSpec((None, HEAD_DIM, rows), lambda h: (h + at_state, 0, 0)),
    ]
    state_shapes = [
        jax.ShapeDtypeStruct((heads, 8, rows), jnp.float32),
        jax.ShapeDtypeStruct((heads, 8, rows), jnp.float32),
        jax.ShapeDtypeStruct((heads, HEAD_DIM, rows), jnp.float32),
    ]
    if final:
        out_specs = pl.BlockSpec((rows, HEAD_DIM), lambda h: (0, h))
        out_shape = jax.ShapeDtypeStruct((rows, heads * HEAD_DIM), jnp.bfloat16)
    else:
        out_specs, out_shape = list(state_specs), list(state_shapes)
        if emit:
            slots = items[0][1].shape[1]
            out_specs.append(
                pl.BlockSpec((len(items), 2, slots, HEAD_DIM), lambda h: (0, 0, 0, h))
            )
            out_shape.append(
                jax.ShapeDtypeStruct((len(items), 2, slots, heads * HEAD_DIM), jnp.bfloat16)
            )

    def kernel(limit_ref, query_ref, *refs):
        given = list(refs)
        if has_state:
            max_ref, sum_ref, mix_ref = given[:3]
            given = given[3:]
        pieces, copied = [], []
        for kind, count in kinds:
            if kind == "text":
                k_ref, v_ref = given[:2]
                given = given[2:]
                pieces.append(
                    (lambda r=k_ref: r[...], lambda r=v_ref: r[...], None, LEAST_PROMPT)
                )
            else:
                r = given.pop(0)
                if kind == "block":
                    copied.append(r)
                if kind == "stack":
                    pieces += [frame_piece(r.at[i]) for i in range(count)]
                else:
                    pieces.append(frame_piece(r))
        outs = given
        q = query_ref[...]
        if has_state:
            carry = (max_ref[0:1], sum_ref[0:1], mix_ref[...])
        else:
            carry = (
                jnp.full((1, rows), NEGATIVE, jnp.float32),
                jnp.zeros((1, rows), jnp.float32),
                jnp.zeros((HEAD_DIM, rows), jnp.float32),
            )

        def run(pieces, carry):
            row_max, weight_sum, mixed = carry
            scores = scores_of(pieces[0][0](), q)
            for i, (_, value_of, limit_of, sure) in enumerate(pieces):
                ahead = scores_of(pieces[i + 1][0](), q) if i + 1 < len(pieces) else None
                count = scores.shape[0]
                slots = lax.broadcasted_iota(jnp.int32, (count - sure, rows), 0) + sure
                limit = limit_ref[0] if limit_of is None else limit_of()
                tail = jnp.where(slots < limit, scores[sure:], NEGATIVE)
                scores = jnp.concatenate([scores[:sure], tail], axis=0)
                new_max = jnp.maximum(row_max, jnp.max(scores, axis=0, keepdims=True))
                base = new_max * LOG2_SCALE
                weights = jnp.exp2(scores * LOG2_SCALE - base)
                shrink = jnp.exp2(row_max * LOG2_SCALE - base)
                columns = jnp.concatenate(
                    [value_of().T, jnp.ones((16, count), jnp.bfloat16)], axis=0
                )
                added = jnp.dot(
                    columns, weights.astype(jnp.bfloat16), preferred_element_type=jnp.float32
                )
                weight_sum = weight_sum * shrink + added[HEAD_DIM : HEAD_DIM + 1]
                mixed = mixed * shrink + added[:HEAD_DIM]
                row_max = new_max
                scores = ahead
            return row_max, weight_sum, mixed

        for i, r in enumerate(copied):
            outs[3][i] = r[...]
        carry = run(pieces, carry)
        row_max, weight_sum, mixed = carry
        if final:
            outs[0][...] = (mixed / weight_sum).T.astype(jnp.bfloat16)
        else:
            outs[0][...] = jnp.broadcast_to(row_max, (8, rows))
            outs[1][...] = jnp.broadcast_to(weight_sum, (8, rows))
            outs[2][...] = mixed

    keys_total = sum(512 if k == "text" else n * FRAME_SLOTS for k, n in kinds)
    flops = 4 * rows * keys_total * HEAD_DIM * heads
    return pl.pallas_call(
        kernel,
        grid=(heads,),
        in_specs=[
            pl.BlockSpec(memory_space=pltpu.SMEM),
            pl.BlockSpec((rows, HEAD_DIM), lambda h: (0, h + first)),
            *(given_specs if has_state else []),
            *specs,
        ],
        out_specs=out_specs,
        out_shape=out_shape,
        compiler_params=pltpu.CompilerParams(vmem_limit_bytes=24 << 20),
        cost_estimate=pl.CostEstimate(
            flops=flops * 2, transcendentals=rows * keys_total * heads, bytes_accessed=1 << 20
        ),
    )(limits, query, *(state if has_state else ()), *operands)


def project(place, total, entries, steps, weights, rows, features, final):
    has_total = total is not None

    def kernel(place_ref, *refs):
        given = list(refs)
        total_ref = given.pop(0) if has_total else None
        h = pl.program_id(0)
        north = place_ref[0] == 0
        result = None
        for _ in entries:
            a, w = given[:8], given[8:16]
            given = given[16:]
            blocks = [a[0][...], a[1][...]]
            for x, y in ((2, 3), (4, 5), (6, 7)):
                blocks.append(jnp.where(north, a[x][...], a[y][...]))
            for x, y in ((2, 3), (4, 5), (6, 7)):
                blocks.append(jnp.where(north, a[y][...], a[x][...]))
            part = jnp.dot(
                jnp.concatenate(blocks, axis=1),
                jnp.concatenate([r[...] for r in w], axis=0),
                preferred_element_type=jnp.float32,
            )
            result = part if result is None else result + part
        if final:
            result = (total_ref[...] + result).astype(jnp.bfloat16)
            lower, upper = result[:, : features // 2], result[:, features // 2 :]
            given[0][...] = jnp.where(place_ref[1] == 0, lower, upper)
            given[1][...] = jnp.where(place_ref[1] == 0, upper, lower)
            return
        out = given[0]

        @pl.when(h == 0)
        def _():
            out[...] = result

        if steps > 1:
            @pl.when(h > 0)
            def _():
                out[...] = out[...] + result

    operands, specs = [], []
    for attended, first, at in entries:
        operands += [*attended, *weights]
        specs += [pl.BlockSpec((rows, HEAD_DIM), lambda h, at=at: (0, h + at))] * len(attended)
        specs += [pl.BlockSpec((HEAD_DIM, features), lambda h, first=first: (h + first, 0))] * len(weights)
    whole = pl.BlockSpec((rows, features), lambda h: (0, 0))
    flops = 16 * rows * features * HEAD_DIM * steps * len(entries)
    return pl.pallas_call(
        kernel,
        grid=(steps,),
        in_specs=[
            pl.BlockSpec(memory_space=pltpu.SMEM),
            *([whole] if has_total else []),
            *specs,
        ],
        out_specs=[pl.BlockSpec((rows, features // 2), lambda h: (0, 0))] * 2 if final else whole,
        out_shape=[jax.ShapeDtypeStruct((rows, features // 2), jnp.bfloat16)] * 2
        if final
        else jax.ShapeDtypeStruct((rows, features), jnp.float32),
        compiler_params=pltpu.CompilerParams(vmem_limit_bytes=24 << 20),
        cost_estimate=pl.CostEstimate(flops=flops, transcendentals=0, bytes_accessed=1 << 20),
    )(place, *([total] if has_total else []), *operands)


def step(queries, keys, values, text_keys, text_values, prompt_lengths, frame_counts, out_weight):
    query, text_k, text_v = queries[0], text_keys[0], text_values[0]
    head_total = query.shape[1] // HEAD_DIM
    rows = query.shape[0]
    features = out_weight.shape[1] // lax.axis_size("tp")
    seq = lax.axis_index("seq")
    tp = lax.axis_index("tp")
    cfg = lax.axis_index("cfg")
    core = seq % 2

    def send(x, axis, pairs):
        return lax.ppermute(x, axis, pairs)

    limits = prompt_lengths

    def rows_of(first, heads):
        cols = slice(first * HEAD_DIM, (first + heads) * HEAD_DIM)
        return with_count(jnp.stack([keys[0][:, cols], values[0][:, cols]]), frame_counts[0])

    both_rows = rows_of(0, head_total)
    both_swapped = send(both_rows, "seq", CORE_SWAP)

    x_pos, y_pos = tp % 4, tp // 4

    def columns_for(target):
        return lax.dynamic_slice(out_weight, (0, target * features), (out_weight.shape[0], features))

    got, got_swapped = [], []
    for step in range(4):
        if step == 3:
            target = (1 - y_pos) * 4 + x_pos
        else:
            target = ((y_pos + core) % 2) * 4 + (x_pos + step + 1) % 4
        got.append(send(columns_for(target), ("seq", "tp"), weight_round(step)))
    for step in range(3):
        got_swapped.append(send(got[step], "seq", CORE_SWAP))
    weights = (columns_for(tp), got[3], *got[:3], *got_swapped)

    start_state = attend(
        query,
        limits,
        [("text", (text_k, text_v)), ("all", both_rows), ("all", both_swapped)],
        None,
        False,
        0,
        head_total,
    )

    rings = []
    for g, (first, heads) in enumerate(GROUPS):
        own = rows_of(first, heads)
        forward, backward = [own], [own]
        for _ in range(3):
            forward.append(send(forward[-1], "seq", z_shift(1)))
            backward.append(send(backward[-1], "seq", z_shift(-1)))
        last = send(backward[3], "seq", z_shift(-1)) if g == 1 else send(forward[3], "seq", z_shift(1))
        frames = {"l4": last}
        for i in (1, 2, 3):
            frames["f%d" % i] = forward[i]
            frames["b%d" % i] = backward[i]
        calls = CALLS[g]
        *state, stacked = attend(
            query,
            limits,
            [("block", frames[name]) for name in calls[0]],
            start_state,
            False,
            first,
            heads,
            first,
            True,
        )
        frames["sn"] = send(stacked, "seq", CORE_SWAP)
        for name in sum(calls[1:], ()):
            if name not in frames:
                frames[name] = send(frames[name[1:]], "seq", CORE_SWAP)
        rings.append((state, frames))

    gathered = []
    place = jnp.stack([core, cfg]).astype(jnp.int32)
    for g, ((first, heads), (state, frames)) in enumerate(zip(GROUPS, rings)):
        for i, names in enumerate(CALLS[g][1:]):
            items = [("stack" if name == "sn" else "last", frames[name]) for name in names]
            final = i + 2 == len(CALLS[g])
            state = attend(query, limits, items, state, final, first, heads)
        mine = state

        def near_tp(x, dy, dx):
            return send(x, "tp", tp_shift(dy, dx))

        across = near_tp(mine, 1, 0)
        left = near_tp(mine, 0, 1)
        right = near_tp(mine, 0, -1)
        left_a = near_tp(across, 0, 1)
        if g == 0:
            right_a = near_tp(right, 1, 0)
            far = near_tp(right, 0, -1)
            far_a = near_tp(far, 1, 0)
        else:
            right_a = near_tp(across, 0, -1)
            far = near_tp(left, 0, 1)
            far_a = near_tp(right_a, 0, -1)
        attended = [mine, across, left, left_a, far, far_a, right, right_a]
        gathered.append(attended)
    total = project(place, None, [(gathered[0], 0, 0)], GROUPS[0][1], weights, rows, features, False)
    first, heads = GROUPS[1]
    entries = [(gathered[1], first + i, i) for i in range(heads)]
    total = project(place, total, entries, 1, weights, rows, features, True)

    half = features // 2
    kept, leaving = total
    given = send(leaving, "cfg", [(0, 1), (1, 0)])
    conditional = jnp.where(cfg == 0, kept, given).astype(jnp.float32)
    unconditional = jnp.where(cfg == 0, given, kept).astype(jnp.float32)
    guided = unconditional + GUIDANCE * (conditional - unconditional)
    token_weights = (jnp.arange(rows, dtype=jnp.int32) < frame_counts[0]).astype(jnp.float32)[:, None]

    def local_sum(field):
        return jnp.sum(field * token_weights, axis=0)

    sums = jnp.stack(
        [
            local_sum(guided),
            local_sum(guided * guided),
            local_sum(conditional),
            local_sum(conditional * conditional),
            jnp.broadcast_to(frame_counts.astype(jnp.float32), (half,)),
        ]
    )
    for bits in ((1, 2, 3), (4, 8, 12)):
        sums = sum([send(sums, "seq", [(i, i ^ b) for i in range(16)]) for b in bits], sums)
    valid_total = sums[4]
    guided_mean = sums[0] / valid_total
    guided_var = sums[1] / valid_total - guided_mean * guided_mean
    cond_mean = sums[2] / valid_total
    cond_var = sums[3] / valid_total - cond_mean * cond_mean
    std_ratio = jnp.sqrt((cond_var + 1.0) / (guided_var + 1.0))
    factor = RESCALE * std_ratio + (1.0 - RESCALE)
    return (guided_mean + (guided - guided_mean) * factor).astype(jnp.bfloat16)


def solution(mesh):
    placed = (
        P("cfg", "seq", "tp"),
        P("cfg", "seq", "tp"),
        P("cfg", "seq", "tp"),
        P("cfg", None, "tp"),
        P("cfg", None, "tp"),
        P("cfg"),
        P("seq"),
        P("tp", None),
    )
    return jax.shard_map(step, mesh=mesh, in_specs=placed, out_specs=P("seq", ("tp", "cfg")), check_vma=False)
```
